256 devices in a mesh: segment: 8 (over y, core), shard: 32 (over x, z).
Axes of the slice: x: 4, y: 4, z: 8, core: 2. Of those that a mesh axis runs over, the one named last changes fastest.
Arguments:
- buffer: bfloat16 [16, 18432, 2304], P('segment', 'shard'), may hold values from -6 to 6
- right_basis: bfloat16 [16, 2304, 256], P('segment', 'shard'), may hold values from -0.125 to 0.125
- layer_count: int32 [8], P('segment'), may hold values from 1 to 2, as said below
Outputs:
- momentum_out: bfloat16 [16, 18432, 2304], P('segment', 'shard')
- left_step: bfloat16 [16, 18432, 256], P('segment', 'shard')
- right_step: float32 [16, 2304, 256], P('segment', 'shard')
The draws below stay inside these ranges and needn't reach their ends.
Inputs may be any that keep to these rules, and one draw needn't show every extreme that they name: `layer_count`: each segment uses between 1 and 2 slots; some segment uses 2 and some segment uses 1.
All inputs are finite; a program needn't handle non-finite values.
Results may differ from the reference program's by a relative error of at most 0.0024.
Values may be sent and summed in bfloat16 or wider, within the bound.
No kernel may reach another device: no remote copies, remote signals or barrier semaphores. Data moves between devices by JAX's collectives and lax.ppermute only.
A program may use at most 64 MiB of HBM per device.

```python
import math
import jax
import jax.numpy as jnp
from jax import lax

ROWS = 18432
COLS = 2304
RANK = 256
SLOTS = 2
LAYER_SLOTS = 16
N_SEGMENT = 8
N_SHARD = 32


def draw_buffer(key, part):
    base = jax.random.fold_in(key, 11)
    first, second = jax.random.split(base, 2)
    rows_dev = ROWS // N_SHARD
    noise = jnp.clip(jax.random.normal(first, (LAYER_SLOTS, N_SHARD, rows_dev, COLS), jnp.float32), -4.0, 4.0)
    logs = jax.random.uniform(second, (LAYER_SLOTS, N_SHARD, 1, 1), jnp.float32, math.log(0.03), math.log(1.0))
    values = jnp.clip(noise * jnp.exp(logs), -6.0, 6.0)
    return values.reshape(LAYER_SLOTS, ROWS, COLS).astype(jnp.bfloat16)


def draw_layer_count(key, part):
    base = jax.random.fold_in(key, 23)
    first, second, third = jax.random.split(base, 3)
    counts = jax.random.randint(first, (N_SEGMENT,), 1, SLOTS + 1)
    fullest = jax.random.randint(second, (), 0, N_SEGMENT)
    lightest = (fullest + 1 + jax.random.randint(third, (), 0, N_SEGMENT - 1)) % N_SEGMENT
    counts = counts.at[fullest].set(SLOTS)
    counts = counts.at[lightest].set(1)
    return counts.astype(jnp.int32)


def shard_levels(rng, shape, pieces, smallest, high):
    def one(dim, blocks):
        steps = jax.random.uniform(jax.random.fold_in(jax.random.fold_in(rng, 6), dim), (blocks,), jnp.float32, smallest / len(pieces), high / len(pieces))
        return jnp.repeat(jnp.exp(steps), shape[dim] // blocks).reshape((-1,) + (1,) * (len(shape) - dim - 1))

    level = one(*pieces[0])
    for cut in pieces[1:]:
        level = level * one(*cut)
    return level


def bell_draw(key, dims, width, reach, pieces=(), kind=jnp.bfloat16):
    gain = shard_levels(key, dims, pieces, -0.22, 0.18) if pieces else 1.0
    values = jax.random.normal(key, dims, jnp.float32) * width * gain
    return jnp.minimum(jnp.maximum(values, -reach), reach).astype(kind)


def setup_inputs(seed: int = 0) -> dict:
    streams_of = jax.random.split(jax.random.key(seed), 4)
    buffer = draw_buffer(jax.random.fold_in(streams_of[3], 71), 0)
    right_basis = bell_draw(streams_of[1], (LAYER_SLOTS, COLS, RANK), COLS ** -0.5, 0.125, ((0, 8), (1, 32)))
    layer_count = draw_layer_count(jax.random.fold_in(streams_of[3], 71), 0)
    return dict(buffer=buffer, right_basis=right_basis, layer_count=layer_count)


MOMENTUM = 0.9
CLIP_RMS = 0.35
SQUARE_FLOOR = 0.0625

def one_layer(pair):
    block, basis = pair
    proj = jnp.dot(block.astype(jnp.float32), basis.astype(jnp.float32), preferred_element_type=jnp.float32)
    gram = jnp.dot(proj.T, proj, precision=lax.Precision.HIGHEST)
    lower = jnp.linalg.cholesky(gram)
    ortho = jax.scipy.linalg.solve_triangular(lower, proj.T, lower=True).T
    half_left = ortho.astype(jnp.bfloat16)
    right = jnp.dot(block.T.astype(jnp.float32), half_left.astype(jnp.float32), preferred_element_type=jnp.float32)
    half_right = right.astype(jnp.bfloat16)
    correction = jnp.dot(half_left.astype(jnp.float32), half_right.T.astype(jnp.float32), preferred_element_type=jnp.float32)
    moment = (block.astype(jnp.float32) - (1.0 - MOMENTUM) * correction).astype(jnp.bfloat16)
    colsq = lax.optimization_barrier(jnp.sum(right * right, axis=0, keepdims=True))
    scaled = right * (math.sqrt(COLS) * lax.rsqrt(colsq + 1.0))
    squares = jnp.sum(jnp.square(block.astype(jnp.float32)))
    return (moment, ortho, scaled, squares)

def reference(buffer, right_basis, layer_count):
    moment, ortho, scaled, squares = lax.map(one_layer, (buffer, right_basis))
    slot_ids = jnp.arange(LAYER_SLOTS, dtype=jnp.int32)
    used = slot_ids % SLOTS < layer_count[slot_ids // SLOTS]
    total_sq = jnp.sum(jnp.where(used, squares, jnp.float32(0.0)))
    elements = jnp.sum(layer_count).astype(jnp.float32) * jnp.float32(ROWS * COLS)
    clip = jnp.minimum(jnp.float32(1.0), CLIP_RMS * lax.rsqrt(jnp.maximum(total_sq / elements, SQUARE_FLOOR)))
    keep = used[:, None, None]
    momentum_out = jnp.where(keep, moment, jnp.zeros_like(moment))
    left_step = jnp.where(keep, clip * math.sqrt(ROWS) * ortho, jnp.float32(0.0)).astype(jnp.bfloat16)
    right_step = jnp.where(keep, scaled, jnp.float32(0.0))
    return (momentum_out, left_step, right_step)
```

```python
import math

import jax
import jax.numpy as jnp
from jax import lax
from jax.experimental import pallas as pl
from jax.experimental.pallas import tpu as pltpu
from jax.sharding import Mesh
from jax.sharding import PartitionSpec as P

SEG = ("segment_0", "segment_1")
X = "shard_0"
Z = "shard_1"
SHARD = (X, Z)

MOMENTUM = 0.9
CLIP_RMS = 0.35
SQUARE_FLOOR = 0.0625
BLOCK = 16
F32 = jnp.float32
BF16 = jnp.bfloat16


def exchange(blocks, axis):
    return lax.all_to_all(blocks, axis, split_axis=0, concat_axis=0, tiled=True)


def spread(value, axis):
    return exchange(jnp.broadcast_to(value, (lax.axis_size(axis), *value.shape)), axis)


def whole_rows(shard):
    slots, rows, rank = shard.shape
    line = spread(shard, Z)
    plane = spread(line, X)
    return plane.reshape(-1, slots, rows, rank).transpose(1, 0, 2, 3).reshape(slots, -1, rank)


def inverse_factor_kernel(gram_ref, out_ref, work_ref):
    slots, n, _ = gram_ref.shape
    b = BLOCK
    for s in range(slots):
        row = lax.broadcasted_iota(jnp.int32, (n, n), 0)
        col = lax.broadcasted_iota(jnp.int32, (n, n), 1)
        work_ref[s, :, :n] = gram_ref[s]
        work_ref[s, :, n:] = (row == col).astype(F32)
    sub = lax.broadcasted_iota(jnp.int32, (b, 128), 0)
    for j in range(n // b):
        lo, hi = j * b, (j + 1) * b
        panels = []
        cols = []
        for s in range(slots):
            panel = work_ref[s, lo:hi, :]
            panels.append(panel)
            cols.append([jnp.broadcast_to(panel[:, lo + k : lo + k + 1], (b, 128)) for k in range(b)])
        for k in range(b):
            for s in range(slots):
                c = cols[s]
                inv = lax.rsqrt(jnp.broadcast_to(c[k][k : k + 1], (b, 128)))
                scaled = c[k] * inv
                below = jnp.where(sub > k, scaled, 0.0)
                for i in range(k + 1, b):
                    c[i] = c[i] - below * jnp.broadcast_to(scaled[i : i + 1], (b, 128))
                p = panels[s]
                inv_row = jnp.concatenate([inv[:1]] * (2 * n // 128), axis=1)
                pivot = p[k : k + 1] * inv_row
                below_all = jnp.concatenate([below] * (2 * n // 128), axis=1)
                at_k = jnp.concatenate([sub == k] * (2 * n // 128), axis=1)
                pivot_all = jnp.broadcast_to(pivot, (b, 2 * n))
                panels[s] = jnp.where(at_k, pivot_all, p - below_all * pivot_all)
        for s in range(slots):
            work_ref[s, lo:hi, :] = panels[s]
            if hi < n:
                tail = panels[s][:, hi:n]
                update = lax.dot_general(
                    tail, panels[s], (((0,), (0,)), ((), ())),
                    precision=lax.Precision.HIGHEST, preferred_element_type=F32,
                )
                work_ref[s, hi:, :] = work_ref[s, hi:, :] - update
    for s in range(slots):
        out_ref[s] = work_ref[s, :, n:]


def inverse_factor(gram):
    slots, n, _ = gram.shape
    return pl.pallas_call(
        inverse_factor_kernel,
        out_shape=jax.ShapeDtypeStruct(gram.shape, F32),
        scratch_shapes=[pltpu.VMEM((slots, n, 2 * n), F32)],
        in_specs=[pl.BlockSpec(memory_space=pltpu.VMEM)],
        out_specs=pl.BlockSpec(memory_space=pltpu.VMEM),
        compiler_params=pltpu.CompilerParams(vmem_limit_bytes=16 << 20),
        name="inverse_factor",
    )(gram)


def body(buffer, right_basis, layer_count):
    slots, rows_dev, cols = buffer.shape
    rank = right_basis.shape[-1]
    devices = lax.axis_size(SHARD)
    near, far = lax.axis_size(Z), lax.axis_size(X)
    rows_all = rows_dev * devices
    width = cols // devices
    count = layer_count[0]
    used = jnp.arange(slots, dtype=jnp.int32) < count
    keep = used[:, None, None]

    basis = whole_rows(right_basis)
    proj = jnp.einsum("kij,kjr->kir", buffer, basis, preferred_element_type=F32)
    gram = jnp.einsum("kir,kis->krs", proj, proj, precision=lax.Precision.HIGHEST)
    per_slot = jnp.sum(jnp.square(buffer.astype(F32)), axis=(1, 2))
    row = lax.broadcasted_iota(jnp.int32, gram.shape, 1)
    col = lax.broadcasted_iota(jnp.int32, gram.shape, 2)
    gram = jnp.where((row == 0) & (col == rank - 1), per_slot[:, None, None], gram)
    part = exchange(gram.reshape(devices, -1, rank), SHARD).sum(axis=0)
    gram = spread(part, SHARD).reshape(slots, rank, rank)
    squares = jnp.sum(jnp.where(used, gram[:, 0, rank - 1], 0.0))
    elements = count.astype(F32) * float(rows_all * cols)
    gram = jnp.where((row == 0) & (col == rank - 1), gram[:, rank - 1 :, :1], gram)

    lane = lax.broadcasted_iota(jnp.int32, (8, 128), 1)
    both = jnp.where(lane == 0, squares, elements)
    totals = spread(both, SEG)[:, 0, :2].sum(axis=0)
    clip = jnp.minimum(1.0, CLIP_RMS * lax.rsqrt(jnp.maximum(totals[0] / totals[1], SQUARE_FLOOR)))

    inverse = inverse_factor(gram)
    ortho = jnp.einsum("kir,ksr->kis", proj, inverse, precision=lax.Precision.HIGHEST)
    half_left = ortho.astype(BF16)
    left = jnp.where(keep, clip * math.sqrt(rows_all) * ortho, 0.0).astype(BF16)

    partial = jnp.einsum("kij,kir->kjr", buffer, half_left, preferred_element_type=F32)
    partial = partial.astype(BF16).reshape(slots, far, near * width, rank).transpose(1, 0, 2, 3)
    line = exchange(partial, X).astype(F32).sum(axis=0)
    line = line.reshape(slots, near, width, rank).transpose(1, 0, 2, 3)
    right = exchange(line, Z).sum(axis=0)
    half_right = whole_rows(right.astype(BF16))
    colsq = jnp.sum(jnp.square(half_right.astype(F32)), axis=1, keepdims=True)
    right_step = jnp.where(keep, right * (math.sqrt(cols) * lax.rsqrt(colsq + 1.0)), 0.0)

    correction = jnp.einsum("kir,kjr->kij", half_left, half_right, preferred_element_type=F32)
    moment = jnp.where(keep, buffer - (1.0 - MOMENTUM) * correction, 0.0).astype(BF16)
    return moment, left, right_step


def solution(mesh):
    split = Mesh(mesh.devices.reshape(4, 2, 4, 8), (*SEG, *SHARD))
    specs = (P(SEG, SHARD, None), P(SEG, SHARD, None), P(SEG))
    outs = (P(SEG, SHARD, None),) * 3
    return jax.shard_map(body, mesh=split, in_specs=specs, out_specs=outs, check_vma=False)
```

```python
import math

import jax
import jax.numpy as jnp
from jax import lax
from jax.experimental import pallas as pl
from jax.experimental.pallas import tpu as pltpu
from jax.sharding import Mesh
from jax.sharding import PartitionSpec as P

SEG = ("segment_0", "segment_1")
X = "x"
FAR_Z = "z_far"
NEAR_Z = "z_near"
SHARD = (X, FAR_Z, NEAR_Z)
PLANE = (X, NEAR_Z)

MOMENTUM = 0.9
CLIP_RMS = 0.35
SQUARE_FLOOR = 0.0625
BLOCK = 16
F32 = jnp.float32
BF16 = jnp.bfloat16


def exchange(blocks, axis):
    return lax.all_to_all(blocks, axis, split_axis=0, concat_axis=0, tiled=True)


def spread(value, axis):
    return exchange(jnp.broadcast_to(value, (lax.axis_size(axis), *value.shape)), axis)


def whole_rows(shard):
    slots, rows, rank = shard.shape
    plane = spread(spread(shard, FAR_Z), PLANE)
    plane = plane.reshape(lax.axis_size(X), lax.axis_size(NEAR_Z), -1, slots, rows, rank)
    return plane.transpose(3, 0, 2, 1, 4, 5).reshape(slots, -1, rank)


def summed_rows(partial):
    slots, lines, rank = partial.shape
    sizes = [lax.axis_size(a) for a in SHARD]
    blocks = partial.reshape(slots, *sizes, -1, rank).transpose(1, 3, 2, 0, 4, 5)
    blocks = blocks.reshape(sizes[0] * sizes[2], *blocks.shape[2:]).astype(BF16)
    line = exchange(blocks, PLANE).astype(F32).sum(axis=0)
    return exchange(line, FAR_Z).sum(axis=0)


def inverse_factor_kernel(gram_ref, out_ref, work_ref):
    slots, n, _ = gram_ref.shape
    b = BLOCK
    for s in range(slots):
        row = lax.broadcasted_iota(jnp.int32, (n, n), 0)
        col = lax.broadcasted_iota(jnp.int32, (n, n), 1)
        work_ref[s, :, :n] = gram_ref[s]
        work_ref[s, :, n:] = (row == col).astype(F32)
    sub = lax.broadcasted_iota(jnp.int32, (b, 128), 0)
    for j in range(n // b):
        lo, hi = j * b, (j + 1) * b
        panels = []
        cols = []
        for s in range(slots):
            panel = work_ref[s, lo:hi, :]
            panels.append(panel)
            cols.append([jnp.broadcast_to(panel[:, lo + k : lo + k + 1], (b, 128)) for k in range(b)])
        for k in range(b):
            for s in range(slots):
                c = cols[s]
                inv = lax.rsqrt(jnp.broadcast_to(c[k][k : k + 1], (b, 128)))
                scaled = c[k] * inv
                below = jnp.where(sub > k, scaled, 0.0)
                for i in range(k + 1, b):
                    c[i] = c[i] - below * jnp.broadcast_to(scaled[i : i + 1], (b, 128))
                p = panels[s]
                inv_row = jnp.concatenate([inv[:1]] * (2 * n // 128), axis=1)
                pivot = p[k : k + 1] * inv_row
                below_all = jnp.concatenate([below] * (2 * n // 128), axis=1)
                at_k = jnp.concatenate([sub == k] * (2 * n // 128), axis=1)
                pivot_all = jnp.broadcast_to(pivot, (b, 2 * n))
                panels[s] = jnp.where(at_k, pivot_all, p - below_all * pivot_all)
        for s in range(slots):
            work_ref[s, lo:hi, :] = panels[s]
            if hi < n:
                tail = panels[s][:, hi:n]
                update = lax.dot_general(
                    tail, panels[s], (((0,), (0,)), ((), ())),
                    precision=lax.Precision.HIGHEST, preferred_element_type=F32,
                )
                work_ref[s, hi:, :] = work_ref[s, hi:, :] - update
    for s in range(slots):
        out_ref[s] = work_ref[s, :, n:]


def inverse_factor(gram):
    slots, n, _ = gram.shape
    return pl.pallas_call(
        inverse_factor_kernel,
        out_shape=jax.ShapeDtypeStruct(gram.shape, F32),
        scratch_shapes=[pltpu.VMEM((slots, n, 2 * n), F32)],
        in_specs=[pl.BlockSpec(memory_space=pltpu.VMEM)],
        out_specs=pl.BlockSpec(memory_space=pltpu.VMEM),
        compiler_params=pltpu.CompilerParams(vmem_limit_bytes=16 << 20),
        name="inverse_factor",
    )(gram)


def body(buffer, right_basis, layer_count):
    slots, rows_dev, cols = buffer.shape
    rank = right_basis.shape[-1]
    devices = lax.axis_size(SHARD)
    rows_all = rows_dev * devices
    count = layer_count[0]
    used = jnp.arange(slots, dtype=jnp.int32) < count
    keep = used[:, None, None]

    basis = whole_rows(right_basis)
    proj = jnp.einsum("kij,kjr->kir", buffer, basis, preferred_element_type=F32)
    gram = jnp.einsum("kir,kis->krs", proj, proj, precision=lax.Precision.HIGHEST)
    per_slot = jnp.sum(jnp.square(buffer.astype(F32)), axis=(1, 2))
    row = lax.broadcasted_iota(jnp.int32, gram.shape, 1)
    col = lax.broadcasted_iota(jnp.int32, gram.shape, 2)
    gram = jnp.where((row == 0) & (col == rank - 1), per_slot[:, None, None], gram)
    part = exchange(gram.reshape(devices, -1, rank), SHARD).sum(axis=0)
    gram = spread(part, SHARD).reshape(slots, rank, rank)
    squares = jnp.sum(jnp.where(used, gram[:, 0, rank - 1], 0.0))
    elements = count.astype(F32) * float(rows_all * cols)
    gram = jnp.where((row == 0) & (col == rank - 1), gram[:, rank - 1 :, :1], gram)

    lane = lax.broadcasted_iota(jnp.int32, (8, 128), 1)
    both = jnp.where(lane == 0, squares, elements)
    totals = spread(both, SEG)[:, 0, :2].sum(axis=0)
    clip = jnp.minimum(1.0, CLIP_RMS * lax.rsqrt(jnp.maximum(totals[0] / totals[1], SQUARE_FLOOR)))

    inverse = inverse_factor(gram)
    ortho = jnp.einsum("kir,ksr->kis", proj, inverse, precision=lax.Precision.HIGHEST)
    half_left = ortho.astype(BF16)
    left = jnp.where(keep, clip * math.sqrt(rows_all) * ortho, 0.0).astype(BF16)

    partial = jnp.einsum("kij,kir->kjr", buffer, half_left, preferred_element_type=F32)
    right = summed_rows(partial)
    half_right = whole_rows(right.astype(BF16))
    colsq = jnp.sum(jnp.square(half_right.astype(F32)), axis=1, keepdims=True)
    right_step = jnp.where(keep, right * (math.sqrt(cols) * lax.rsqrt(colsq + 1.0)), 0.0)

    correction = jnp.einsum("kir,kjr->kij", half_left, half_right, preferred_element_type=F32)
    moment = jnp.where(keep, buffer - (1.0 - MOMENTUM) * correction, 0.0).astype(BF16)
    return moment, left, right_step


def solution(mesh):
    split = Mesh(mesh.devices.reshape(4, 2, 4, 4, 2), (*SEG, *SHARD))
    specs = (P(SEG, SHARD, None), P(SEG, SHARD, None), P(SEG))
    outs = (P(SEG, SHARD, None),) * 3
    return jax.shard_map(body, mesh=split, in_specs=specs, out_specs=outs, check_vma=False)
```

```python
import math

import jax
import jax.numpy as jnp
from jax import lax
from jax.experimental import pallas as pl
from jax.experimental.pallas import tpu as pltpu
from jax.sharding import Mesh
from jax.sharding import PartitionSpec as P

SEG = ("segment_0", "segment_1")
X = "x"
FAR_Z = "z_far"
NEAR_Z = "z_near"
SHARD = (X, FAR_Z, NEAR_Z)
PLANE = (X, NEAR_Z)

MOMENTUM = 0.9
CLIP_RMS = 0.35
SQUARE_FLOOR = 0.0625
BLOCK = 16
F32 = jnp.float32
BF16 = jnp.bfloat16


def exchange(blocks, axis):
    return lax.all_to_all(blocks, axis, split_axis=0, concat_axis=0, tiled=True)


def spread(value, axis):
    return exchange(jnp.broadcast_to(value, (lax.axis_size(axis), *value.shape)), axis)


def whole_rows(shard):
    slots, rows, rank = shard.shape
    plane = spread(spread(shard, FAR_Z), PLANE)
    plane = plane.reshape(lax.axis_size(X), lax.axis_size(NEAR_Z), -1, slots, rows, rank)
    return plane.transpose(3, 0, 2, 1, 4, 5).reshape(slots, -1, rank)


def summed_rows(blocks):
    line = exchange(blocks, PLANE).astype(F32).sum(axis=0)
    return exchange(line, FAR_Z).sum(axis=0)


def project_kernel(square_ref, block_ref, basis_ref, proj_ref, gram_ref):
    slot, step = pl.program_id(0), pl.program_id(1)
    proj = jnp.dot(block_ref[0], basis_ref[0], preferred_element_type=F32)
    proj_ref[0] = proj
    gram = lax.dot_general(
        proj, proj, (((0,), (0,)), ((), ())), precision=lax.Precision.HIGHEST, preferred_element_type=F32
    )
    total = jnp.where(step == 0, gram, gram_ref[0] + gram)
    row = lax.broadcasted_iota(jnp.int32, total.shape, 0)
    col = lax.broadcasted_iota(jnp.int32, total.shape, 1)
    corner = (row == 0) & (col == total.shape[1] - 1)
    gram_ref[0] = jnp.where(corner, square_ref[slot], total)


def project(buffer, basis, squares, steps=2):
    slots, rows, cols = buffer.shape
    rank = basis.shape[-1]
    part = rows // steps
    return pl.pallas_call(
        project_kernel,
        grid=(slots, steps),
        in_specs=[
            pl.BlockSpec(memory_space=pltpu.SMEM),
            pl.BlockSpec((1, part, cols), lambda s, i: (s, i, 0)),
            pl.BlockSpec((1, cols, rank), lambda s, i: (s, 0, 0)),
        ],
        out_specs=[
            pl.BlockSpec((1, part, rank), lambda s, i: (s, i, 0)),
            pl.BlockSpec((1, rank, rank), lambda s, i: (s, 0, 0)),
        ],
        out_shape=[
            jax.ShapeDtypeStruct((slots, rows, rank), F32),
            jax.ShapeDtypeStruct((slots, rank, rank), F32),
        ],
        compiler_params=pltpu.CompilerParams(vmem_limit_bytes=24 << 20),
        name="project",
    )(squares, buffer, basis)


def eliminate(work_ref, slots, n):
    b = BLOCK
    tiles = 2 * n // 128
    sub = lax.broadcasted_iota(jnp.int32, (b, 128), 0)
    for j in range(n // b):
        lo, hi = j * b, (j + 1) * b
        panels = []
        cols = []
        for s in range(slots):
            panel = work_ref[s, lo:hi, :]
            panels.append(panel)
            cols.append([jnp.broadcast_to(panel[:, lo + k : lo + k + 1], (b, 128)) for k in range(b)])
        for k in range(b):
            for s in range(slots):
                c = cols[s]
                inv = lax.rsqrt(jnp.broadcast_to(c[k][k : k + 1], (b, 128)))
                scaled = c[k] * inv
                below = jnp.where(sub > k, scaled, 0.0)
                for i in range(k + 1, b):
                    c[i] = c[i] - below * jnp.broadcast_to(scaled[i : i + 1], (b, 128))
                p = panels[s]
                pivot = p[k : k + 1] * jnp.concatenate([inv[:1]] * tiles, axis=1)
                below_all = jnp.concatenate([below] * tiles, axis=1)
                at_k = jnp.concatenate([sub == k] * tiles, axis=1)
                pivot_all = jnp.broadcast_to(pivot, (b, 2 * n))
                panels[s] = jnp.where(at_k, pivot_all, p - below_all * pivot_all)
        for s in range(slots):
            work_ref[s, lo:hi, :] = panels[s]
            if hi < n:
                update = lax.dot_general(
                    panels[s][:, hi:n], panels[s], (((0,), (0,)), ((), ())),
                    precision=lax.Precision.HIGHEST, preferred_element_type=F32,
                )
                work_ref[s, hi:, :] = work_ref[s, hi:, :] - update


def factor_kernel(gram_ref, proj_ref, buffer_ref, ortho_ref, half_ref, blocks_ref, work_ref, block_ref, sum_ref, sems):
    slots, rows, n = proj_ref.shape
    cols = block_ref.shape[-1]
    near_blocks, far, _, width, _ = blocks_ref.shape
    loads = [pltpu.make_async_copy(buffer_ref.at[s], block_ref.at[s], sems.at[s]) for s in range(slots)]
    for load in loads:
        load.start()
    row = lax.broadcasted_iota(jnp.int32, (n, n), 0)
    col = lax.broadcasted_iota(jnp.int32, (n, n), 1)
    for s in range(slots):
        gram = gram_ref[s * n : (s + 1) * n, :]
        mirror = jnp.broadcast_to(gram[n - 1 :, :1], (n, n))
        work_ref[s, :, :n] = jnp.where((row == 0) & (col == n - 1), mirror, gram)
        work_ref[s, :, n:] = (row == col).astype(F32)
    eliminate(work_ref, slots, n)
    for s in range(slots):
        ortho = lax.dot_general(
            proj_ref[s], work_ref[s, :, n:], (((1,), (1,)), ((), ())),
            precision=lax.Precision.HIGHEST, preferred_element_type=F32,
        )
        ortho_ref[s] = ortho
        half_ref[s] = ortho.astype(BF16)
        loads[s].wait()
        half = half_ref[s]
        for c in range(0, cols, n):
            sum_ref[c : c + n, :] = lax.dot_general(
                block_ref[s, :, c : c + n], half, (((0,), (0,)), ((), ())), preferred_element_type=F32
            )
        near = lax.axis_size(NEAR_Z)
        for c in range(cols // width):
            x, z = divmod(c, far * near)
            f, m = divmod(z, near)
            blocks_ref[x * near + m, f, s] = sum_ref[c * width : (c + 1) * width, :].astype(BF16)


def factor(gram, proj, buffer):
    slots, rows, rank = proj.shape
    cols = buffer.shape[-1]
    devices = lax.axis_size(SHARD)
    far = lax.axis_size(FAR_Z)
    vmem = pl.BlockSpec(memory_space=pltpu.VMEM)
    return pl.pallas_call(
        factor_kernel,
        in_specs=[vmem, vmem, pl.BlockSpec(memory_space=pl.ANY)],
        out_specs=[vmem, vmem, vmem],
        out_shape=[
            jax.ShapeDtypeStruct((slots, rows, rank), F32),
            jax.ShapeDtypeStruct((slots, rows, rank), BF16),
            jax.ShapeDtypeStruct((devices // far, far, slots, cols // devices, rank), BF16),
        ],
        scratch_shapes=[
            pltpu.VMEM((slots, rank, 2 * rank), F32),
            pltpu.VMEM((slots, rows, cols), BF16),
            pltpu.VMEM((cols, rank), F32),
            pltpu.SemaphoreType.DMA((slots,)),
        ],
        compiler_params=pltpu.CompilerParams(vmem_limit_bytes=32 << 20),
        name="factor",
    )(gram, proj, buffer)


def body(buffer, right_basis, layer_count):
    slots, rows_dev, cols = buffer.shape
    rank = right_basis.shape[-1]
    devices = lax.axis_size(SHARD)
    rows_all = rows_dev * devices
    count = layer_count[0]
    used = jnp.arange(slots, dtype=jnp.int32) < count
    keep = used[:, None, None]

    basis = whole_rows(right_basis)
    per_slot = jnp.sum(jnp.square(buffer.astype(F32)), axis=(1, 2))
    proj, gram = project(buffer, basis, per_slot)
    part = exchange(gram.reshape(devices, -1, rank), SHARD).sum(axis=0)
    gram = spread(part, SHARD).reshape(slots * rank, rank)
    ortho, half_left, blocks = factor(gram, proj, buffer)
    right = summed_rows(blocks)

    squares = jnp.sum(jnp.where(used, gram[::rank, rank - 1], 0.0))
    elements = count.astype(F32) * float(rows_all * cols)
    totals = lax.psum(jnp.stack([squares, elements]), SEG)
    clip = jnp.minimum(1.0, CLIP_RMS * lax.rsqrt(jnp.maximum(totals[0] / totals[1], SQUARE_FLOOR)))
    left = jnp.where(keep, clip * math.sqrt(rows_all) * ortho, 0.0).astype(BF16)

    half_right = whole_rows(right.astype(BF16))
    colsq = jnp.sum(jnp.square(half_right.astype(F32)), axis=1, keepdims=True)
    right_step = jnp.where(keep, right * (math.sqrt(cols) * lax.rsqrt(colsq + 1.0)), 0.0)

    correction = jnp.einsum("kir,kjr->kij", half_left, half_right, preferred_element_type=F32)
    moment = jnp.where(keep, buffer - (1.0 - MOMENTUM) * correction, 0.0).astype(BF16)
    return moment, left, right_step


def solution(mesh):
    split = Mesh(mesh.devices.reshape(4, 2, 4, 4, 2), (*SEG, *SHARD))
    specs = (P(SEG, SHARD, None), P(SEG, SHARD, None), P(SEG))
    outs = (P(SEG, SHARD, None),) * 3
    return jax.shard_map(body, mesh=split, in_specs=specs, out_specs=outs, check_vma=False)
```

```python
import math

import jax
import jax.numpy as jnp
from jax import lax
from jax.experimental import pallas as pl
from jax.experimental.pallas import tpu as pltpu
from jax.sharding import Mesh
from jax.sharding import PartitionSpec as P

SEG = ("segment_0", "segment_1")
X = "x"
FAR_Z = "z_far"
NEAR_Z = "z_near"
SHARD = (X, FAR_Z, NEAR_Z)
PLANE = (X, NEAR_Z)

MOMENTUM = 0.9
CLIP_RMS = 0.35
SQUARE_FLOOR = 0.0625
BLOCK = 16
F32 = jnp.float32
BF16 = jnp.bfloat16


def exchange(blocks, axis):
    return lax.all_to_all(blocks, axis, split_axis=0, concat_axis=0, tiled=True)


def spread(value, axis):
    return exchange(jnp.broadcast_to(value, (lax.axis_size(axis), *value.shape)), axis)


def whole_rows(shard):
    slots, rows, rank = shard.shape
    plane = spread(spread(shard, FAR_Z), PLANE)
    plane = plane.reshape(lax.axis_size(X), lax.axis_size(NEAR_Z), -1, slots, rows, rank)
    return plane.transpose(3, 0, 2, 1, 4, 5).reshape(slots, -1, rank)


def summed_rows(blocks):
    line = exchange(blocks, PLANE).astype(F32).sum(axis=0)
    return exchange(line, FAR_Z).sum(axis=0)


def halves(value):
    high = value.astype(BF16)
    return high, (value - high.astype(F32)).astype(BF16)


def dot(a, b, dims):
    return lax.dot_general(a, b, (dims, ((), ())), preferred_element_type=F32)


VMEM = pl.BlockSpec(memory_space=pltpu.VMEM)


HBM = pl.BlockSpec(memory_space=pltpu.HBM)


def project_kernel(square_ref, buffer_ref, basis_ref, proj_ref, gram_ref, block_ref, sems):
    slots, rows, n = proj_ref.shape
    parts = sems.shape[1]
    part = rows // parts

    def load(s, i):
        at = pl.ds(i * part, part)
        return pltpu.make_async_copy(buffer_ref.at[s, at], block_ref.at[s, at], sems.at[s, i])

    for s in range(slots):
        for i in range(parts):
            load(s, i).start()
    row = lax.broadcasted_iota(jnp.int32, (n, n), 0)
    col = lax.broadcasted_iota(jnp.int32, (n, n), 1)
    for s in range(slots):
        for i in range(parts):
            load(s, i).wait()
            lines = slice(i * part, (i + 1) * part)
            proj_ref[s, lines, :] = jnp.dot(block_ref[s, lines, :], basis_ref[s], preferred_element_type=F32)
        high, low = halves(proj_ref[s])
        cross = dot(high, low, ((0,), (0,)))
        gram = dot(high, high, ((0,), (0,))) + (dot(low, low, ((0,), (0,))) + (cross + cross.T))
        gram_ref[s] = jnp.where((row == 0) & (col == n - 1), square_ref[s], gram)


def project(buffer, basis, squares, parts=4):
    slots, rows, cols = buffer.shape
    rank = basis.shape[-1]
    return pl.pallas_call(
        project_kernel,
        in_specs=[pl.BlockSpec(memory_space=pltpu.SMEM), HBM, VMEM],
        out_specs=[VMEM, VMEM],
        out_shape=[
            jax.ShapeDtypeStruct((slots, rows, rank), F32),
            jax.ShapeDtypeStruct((slots, rank, rank), F32),
        ],
        scratch_shapes=[pltpu.VMEM((slots, rows, cols), BF16), pltpu.SemaphoreType.DMA((slots, parts))],
        compiler_params=pltpu.CompilerParams(vmem_limit_bytes=24 << 20),
        name="project",
    )(squares, pltpu.with_memory_space_constraint(buffer, pltpu.HBM), basis)


def eliminate(work_ref, slots, n):
    b = BLOCK
    tiles = n // 128
    sub = lax.broadcasted_iota(jnp.int32, (b, 128), 0)
    sub_all = lax.broadcasted_iota(jnp.int32, (b, n), 0)
    lane_all = lax.broadcasted_iota(jnp.int32, (b, n), 1)
    for j in range(n // b):
        lo, hi = j * b, (j + 1) * b
        inside = (lane_all >= lo) & (lane_all < hi)
        panels = []
        cols = []
        for s in range(slots):
            panel = work_ref[s, lo:hi, :]
            cols.append([jnp.broadcast_to(panel[:, lo + k : lo + k + 1], (b, 128)) for k in range(b)])
            panels.append(jnp.where(inside, (lane_all - lo == sub_all).astype(F32), panel))
        for k in range(b):
            for s in range(slots):
                c = cols[s]
                inv = lax.rsqrt(jnp.broadcast_to(c[k][k : k + 1], (b, 128)))
                scaled = c[k] * inv
                below = jnp.where(sub > k, scaled, 0.0)
                for i in range(k + 1, b):
                    c[i] = c[i] - below * jnp.broadcast_to(scaled[i : i + 1], (b, 128))
                p = panels[s]
                pivot = p[k : k + 1] * jnp.concatenate([inv[:1]] * tiles, axis=1)
                below_all = jnp.concatenate([below] * tiles, axis=1)
                pivot_all = jnp.broadcast_to(pivot, (b, n))
                panels[s] = jnp.where(sub_all == k, pivot_all, p - below_all * pivot_all)
        for s in range(slots):
            work_ref[s, lo:hi, :] = panels[s]
            if hi < n:
                update = lax.dot_general(
                    panels[s][:, hi:n], panels[s], (((0,), (0,)), ((), ())),
                    precision=lax.Precision.HIGHEST, preferred_element_type=F32,
                )
                lane = lax.broadcasted_iota(jnp.int32, update.shape, 1)
                old = jnp.where((lane >= lo) & (lane < hi), 0.0, work_ref[s, hi:, :])
                work_ref[s, hi:, :] = old - update


def factor_kernel(gram_ref, proj_ref, buffer_ref, ortho_ref, half_ref, blocks_ref, work_ref, block_ref, sum_ref, sems):
    slots, rows, n = proj_ref.shape
    cols = block_ref.shape[-1]
    far, width = blocks_ref.shape[1], blocks_ref.shape[3]
    near = lax.axis_size(NEAR_Z)
    loads = [pltpu.make_async_copy(buffer_ref.at[s], block_ref.at[s], sems.at[s]) for s in range(slots)]
    for load in loads:
        load.start()
    row = lax.broadcasted_iota(jnp.int32, (n, n), 0)
    col = lax.broadcasted_iota(jnp.int32, (n, n), 1)
    for s in range(slots):
        gram = gram_ref[s * n : (s + 1) * n, :]
        mirror = jnp.broadcast_to(gram[n - 1 :, :1], (n, n))
        work_ref[s] = jnp.where((row == 0) & (col == n - 1), mirror, gram)
    eliminate(work_ref, slots, n)
    for s in range(slots):
        high, low = halves(jnp.where(row >= col, work_ref[s], 0.0))
        proj_high, proj_low = halves(proj_ref[s])
        across = ((1,), (1,))
        ortho = dot(proj_high, high, across) + (dot(proj_high, low, across) + dot(proj_low, high, across))
        ortho_ref[s] = ortho
        half = ortho.astype(BF16)
        half_ref[s] = half
        loads[s].wait()
        for c in range(0, cols, n):
            sum_ref[c : c + n, :] = dot(block_ref[s, :, c : c + n], half, ((0,), (0,)))
        for c in range(cols // width):
            x, z = divmod(c, far * near)
            f, m = divmod(z, near)
            blocks_ref[x * near + m, f, s] = sum_ref[c * width : (c + 1) * width, :].astype(BF16)


def factor(gram, proj, buffer):
    slots, rows, rank = proj.shape
    cols = buffer.shape[-1]
    devices = lax.axis_size(SHARD)
    far = lax.axis_size(FAR_Z)
    return pl.pallas_call(
        factor_kernel,
        in_specs=[VMEM, VMEM, HBM],
        out_specs=[VMEM, VMEM, VMEM],
        out_shape=[
            jax.ShapeDtypeStruct((slots, rows, rank), F32),
            jax.ShapeDtypeStruct((slots, rows, rank), BF16),
            jax.ShapeDtypeStruct((devices // far, far, slots, cols // devices, rank), BF16),
        ],
        scratch_shapes=[
            pltpu.VMEM((slots, rank, rank), F32),
            pltpu.VMEM((slots, rows, cols), BF16),
            pltpu.VMEM((cols, rank), F32),
            pltpu.SemaphoreType.DMA((slots,)),
        ],
        compiler_params=pltpu.CompilerParams(vmem_limit_bytes=32 << 20),
        name="factor",
    )(gram, proj, pltpu.with_memory_space_constraint(buffer, pltpu.HBM))


def body(buffer, right_basis, layer_count):
    slots, rows_dev, cols = buffer.shape
    rank = right_basis.shape[-1]
    devices = lax.axis_size(SHARD)
    rows_all = rows_dev * devices
    count = layer_count[0]
    used = jnp.arange(slots, dtype=jnp.int32) < count
    keep = used[:, None, None]

    basis = whole_rows(right_basis)
    per_slot = jnp.sum(jnp.square(buffer.astype(F32)), axis=(1, 2))
    proj, gram = project(buffer, basis, per_slot)
    part = exchange(gram.reshape(devices, -1, rank), SHARD).sum(axis=0)
    gram = spread(part, SHARD).reshape(slots * rank, rank)
    ortho, half_left, blocks = factor(gram, proj, buffer)
    right = summed_rows(blocks)

    squares = jnp.sum(jnp.where(used, gram[::rank, rank - 1], 0.0))
    elements = count.astype(F32) * float(rows_all * cols)
    totals = lax.psum(jnp.stack([squares, elements]), SEG)
    clip = jnp.minimum(1.0, CLIP_RMS * lax.rsqrt(jnp.maximum(totals[0] / totals[1], SQUARE_FLOOR)))
    left = jnp.where(keep, clip * math.sqrt(rows_all) * ortho, 0.0).astype(BF16)

    right, left = lax.optimization_barrier((right, left))
    half_right = whole_rows(right.astype(BF16))
    colsq = jnp.sum(jnp.square(half_right.astype(F32)), axis=1, keepdims=True)
    right_step = jnp.where(keep, right * (math.sqrt(cols) * lax.rsqrt(colsq + 1.0)), 0.0)

    correction = jnp.einsum("kir,kjr->kij", half_left, half_right, preferred_element_type=F32)
    moment = jnp.where(keep, buffer - (1.0 - MOMENTUM) * correction, 0.0).astype(BF16)
    return moment, left, right_step


def solution(mesh):
    split = Mesh(mesh.devices.reshape(4, 2, 4, 4, 2), (*SEG, *SHARD))
    specs = (P(SEG, SHARD, None), P(SEG, SHARD, None), P(SEG))
    outs = (P(SEG, SHARD, None),) * 3
    return jax.shard_map(body, mesh=split, in_specs=specs, out_specs=outs, check_vma=False)
```

```python
import functools
import math

import jax
import jax.numpy as jnp
from jax import lax
from jax.experimental import pallas as pl
from jax.experimental.pallas import tpu as pltpu
from jax.sharding import Mesh
from jax.sharding import PartitionSpec as P

SEG = ("segment_0", "segment_1")
X = "x"
FAR_Z = "z_far"
NEAR_Z = "z_near"
SHARD = (X, FAR_Z, NEAR_Z)
PLANE = (X, NEAR_Z)

MOMENTUM = 0.9
CLIP_RMS = 0.35
SQUARE_FLOOR = 0.0625
BLOCK = 16
F32 = jnp.float32
BF16 = jnp.bfloat16


def exchange(blocks, axis):
    return lax.all_to_all(blocks, axis, split_axis=0, concat_axis=0, tiled=True)


def spread(value, axis):
    return exchange(jnp.broadcast_to(value, (lax.axis_size(axis), *value.shape)), axis)


def whole_rows(shard):
    slots, rows, rank = shard.shape
    plane = spread(spread(shard, FAR_Z), PLANE)
    plane = plane.reshape(lax.axis_size(X), lax.axis_size(NEAR_Z), -1, slots, rows, rank)
    return plane.transpose(3, 0, 2, 1, 4, 5).reshape(slots, -1, rank)


def halves(value):
    high = value.astype(BF16)
    return high, (value - high.astype(F32)).astype(BF16)


def dot(a, b, dims):
    return lax.dot_general(a, b, (dims, ((), ())), preferred_element_type=F32)


VMEM = pl.BlockSpec(memory_space=pltpu.VMEM)


HBM = pl.BlockSpec(memory_space=pltpu.HBM)


def project_kernel(square_ref, buffer_ref, basis_ref, proj_ref, pack_ref, block_ref, sems):
    slots, rows, n = proj_ref.shape
    parts = sems.shape[1]
    part = rows // parts

    def load(s, i):
        at = pl.ds(i * part, part)
        return pltpu.make_async_copy(buffer_ref.at[s, at], block_ref.at[s, at], sems.at[s, i])

    for s in range(slots):
        for i in range(parts):
            load(s, i).start()
    row = lax.broadcasted_iota(jnp.int32, (n, n), 0)
    col = lax.broadcasted_iota(jnp.int32, (n, n), 1)
    grams = []
    for s in range(slots):
        for i in range(parts):
            load(s, i).wait()
            lines = slice(i * part, (i + 1) * part)
            proj_ref[s, lines, :] = jnp.dot(block_ref[s, lines, :], basis_ref[s], preferred_element_type=F32)
        high, low = halves(proj_ref[s])
        cross = dot(high, low, ((0,), (0,)))
        grams.append(dot(high, high, ((0,), (0,))) + (dot(low, low, ((0,), (0,))) + (cross + cross.T)))
    lower, upper = grams
    pack_ref[:, :n] = jnp.where(row >= col, lower, upper)
    diagonal = jnp.sum(jnp.where(row == col, upper, 0.0), axis=1, keepdims=True)
    row, col = row[:, :128], col[:, :128]
    squares = jnp.where(row == 0, square_ref[0], square_ref[1])
    pack_ref[:, n:] = jnp.where(col == 0, diagonal, jnp.where((col == 1) & (row < slots), squares, 0.0))


def project(buffer, basis, squares, parts=4):
    slots, rows, cols = buffer.shape
    rank = basis.shape[-1]
    return pl.pallas_call(
        project_kernel,
        in_specs=[pl.BlockSpec(memory_space=pltpu.SMEM), HBM, VMEM],
        out_specs=[VMEM, VMEM],
        out_shape=[
            jax.ShapeDtypeStruct((slots, rows, rank), F32),
            jax.ShapeDtypeStruct((rank, rank + 128), F32),
        ],
        scratch_shapes=[pltpu.VMEM((slots, rows, cols), BF16), pltpu.SemaphoreType.DMA((slots, parts))],
        compiler_params=pltpu.CompilerParams(vmem_limit_bytes=24 << 20),
        name="project",
    )(squares, pltpu.with_memory_space_constraint(buffer, pltpu.HBM), basis)


def eliminate(work_ref, slots, n):
    b = BLOCK
    tiles = n // 128
    sub = lax.broadcasted_iota(jnp.int32, (b, 128), 0)
    sub_all = lax.broadcasted_iota(jnp.int32, (b, n), 0)
    lane_all = lax.broadcasted_iota(jnp.int32, (b, n), 1)
    for j in range(n // b):
        lo, hi = j * b, (j + 1) * b
        inside = (lane_all >= lo) & (lane_all < hi)
        panels = []
        cols = []
        for s in range(slots):
            panel = work_ref[s, lo:hi, :]
            cols.append([jnp.broadcast_to(panel[:, lo + k : lo + k + 1], (b, 128)) for k in range(b)])
            panels.append(jnp.where(inside, (lane_all - lo == sub_all).astype(F32), panel))
        for k in range(b):
            for s in range(slots):
                c = cols[s]
                inv = lax.rsqrt(jnp.broadcast_to(c[k][k : k + 1], (b, 128)))
                scaled = c[k] * inv
                below = jnp.where(sub > k, scaled, 0.0)
                for i in range(k + 1, b):
                    c[i] = c[i] - below * jnp.broadcast_to(scaled[i : i + 1], (b, 128))
                p = panels[s]
                pivot = p[k : k + 1] * jnp.concatenate([inv[:1]] * tiles, axis=1)
                below_all = jnp.concatenate([below] * tiles, axis=1)
                pivot_all = jnp.broadcast_to(pivot, (b, n))
                panels[s] = jnp.where(sub_all == k, pivot_all, p - below_all * pivot_all)
        for s in range(slots):
            work_ref[s, lo:hi, :] = panels[s]
            if hi < n:
                update = lax.dot_general(
                    panels[s][:, hi:n], panels[s], (((0,), (0,)), ((), ())),
                    precision=lax.Precision.HIGHEST, preferred_element_type=F32,
                )
                lane = lax.broadcasted_iota(jnp.int32, update.shape, 1)
                old = jnp.where((lane >= lo) & (lane < hi), 0.0, work_ref[s, hi:, :])
                work_ref[s, hi:, :] = old - update


def factor_kernel(near, pack_ref, proj_ref, buffer_ref, ortho_ref, half_ref, blocks_ref, work_ref, block_ref, sum_ref, sems):
    slots, rows, n = proj_ref.shape
    cols = block_ref.shape[-1]
    far, width = blocks_ref.shape[1], blocks_ref.shape[3]
    loads = [pltpu.make_async_copy(buffer_ref.at[s], block_ref.at[s], sems.at[s]) for s in range(slots)]
    for load in loads:
        load.start()
    row = lax.broadcasted_iota(jnp.int32, (n, n), 0)
    col = lax.broadcasted_iota(jnp.int32, (n, n), 1)
    pack = pack_ref[:, :n]
    turned = pack.T
    work_ref[0] = jnp.where(row >= col, pack, turned)
    diagonal = jnp.broadcast_to(pack_ref[:, n : n + 1], (n, n))
    work_ref[1] = jnp.where(row < col, pack, jnp.where(row > col, turned, diagonal))
    eliminate(work_ref, slots, n)
    for s in range(slots):
        high, low = halves(jnp.where(row >= col, work_ref[s], 0.0))
        proj_high, proj_low = halves(proj_ref[s])
        across = ((1,), (1,))
        ortho = dot(proj_high, high, across) + (dot(proj_high, low, across) + dot(proj_low, high, across))
        ortho_ref[s] = ortho
        half = ortho.astype(BF16)
        half_ref[s] = half
        loads[s].wait()
        for c in range(0, cols, n):
            sum_ref[c : c + n, :] = dot(block_ref[s, :, c : c + n], half, ((0,), (0,)))
        for c in range(cols // width):
            x, z = divmod(c, far * near)
            f, m = divmod(z, near)
            blocks_ref[x * near + m, f, s] = sum_ref[c * width : (c + 1) * width, :].astype(BF16)


def factor(pack, proj, buffer, far, near, devices):
    slots, rows, rank = proj.shape
    cols = buffer.shape[-1]
    return pl.pallas_call(
        functools.partial(factor_kernel, near),
        in_specs=[VMEM, VMEM, HBM],
        out_specs=[VMEM, VMEM, VMEM],
        out_shape=[
            jax.ShapeDtypeStruct((slots, rows, rank), F32),
            jax.ShapeDtypeStruct((slots, rows, rank), BF16),
            jax.ShapeDtypeStruct((devices // far, far, slots, cols // devices, rank), BF16),
        ],
        scratch_shapes=[
            pltpu.VMEM((slots, rank, rank), F32),
            pltpu.VMEM((slots, rows, cols), BF16),
            pltpu.VMEM((cols, rank), F32),
            pltpu.SemaphoreType.DMA((slots,)),
        ],
        compiler_params=pltpu.CompilerParams(vmem_limit_bytes=32 << 20),
        name="factor",
    )(pack, proj, pltpu.with_memory_space_constraint(buffer, pltpu.HBM))


def add_kernel(blocks_ref, out_ref):
    for i in range(blocks_ref.shape[1]):
        total = blocks_ref[0, i].astype(F32)
        for j in range(1, blocks_ref.shape[0]):
            total = total + blocks_ref[j, i].astype(F32)
        out_ref[i] = total.astype(BF16)


def added(blocks):
    return pl.pallas_call(
        add_kernel,
        in_specs=[VMEM],
        out_specs=VMEM,
        out_shape=jax.ShapeDtypeStruct(blocks.shape[1:], BF16),
        compiler_params=pltpu.CompilerParams(vmem_limit_bytes=12 << 20),
        name="added",
    )(blocks)


def body(buffer, right_basis, layer_count):
    slots, rows_dev, cols = buffer.shape
    rank = right_basis.shape[-1]
    devices = lax.axis_size(SHARD)
    rows_all = rows_dev * devices
    count = layer_count[0]
    used = jnp.arange(slots, dtype=jnp.int32) < count
    keep = used[:, None, None]

    basis = whole_rows(right_basis)
    per_slot = jnp.sum(jnp.square(buffer.astype(F32)), axis=(1, 2))
    proj, pack = project(buffer, basis, per_slot)
    part = exchange(pack.reshape(devices, -1, pack.shape[-1]), SHARD).sum(axis=0)
    pack = spread(part, SHARD).reshape(pack.shape)
    sizes = lax.axis_size(FAR_Z), lax.axis_size(NEAR_Z), devices
    ortho, half_left, blocks = factor(pack, proj, buffer, *sizes)
    line = added(exchange(blocks, PLANE))

    squares = jnp.sum(jnp.where(used, pack[:slots, rank + 1], 0.0))
    elements = count.astype(F32) * float(rows_all * cols)
    totals = lax.psum(jnp.stack([squares, elements]), SEG)
    clip = jnp.minimum(1.0, CLIP_RMS * lax.rsqrt(jnp.maximum(totals[0] / totals[1], SQUARE_FLOOR)))
    left = jnp.where(keep, clip * math.sqrt(rows_all) * ortho, 0.0).astype(BF16)

    line, left = lax.optimization_barrier((line, left))
    right = exchange(line, FAR_Z).astype(F32).sum(axis=0)
    half_right = whole_rows(right.astype(BF16))
    colsq = jnp.sum(jnp.square(half_right.astype(F32)), axis=1, keepdims=True)
    right_step = jnp.where(keep, right * (math.sqrt(cols) * lax.rsqrt(colsq + 1.0)), 0.0)

    correction = jnp.einsum("kir,kjr->kij", half_left, half_right, preferred_element_type=F32)
    moment = jnp.where(keep, buffer - (1.0 - MOMENTUM) * correction, 0.0).astype(BF16)
    return moment, left, right_step


def solution(mesh):
    split = Mesh(mesh.devices.reshape(4, 2, 4, 4, 2), (*SEG, *SHARD))
    specs = (P(SEG, SHARD, None), P(SEG, SHARD, None), P(SEG))
    outs = (P(SEG, SHARD, None),) * 3
    return jax.shard_map(body, mesh=split, in_specs=specs, out_specs=outs, check_vma=False)
```

```python
import functools
import math

import jax
import jax.numpy as jnp
from jax import lax
from jax.experimental import pallas as pl
from jax.experimental.pallas import tpu as pltpu
from jax.sharding import Mesh
from jax.sharding import PartitionSpec as P

SEG = ("segment_0", "segment_1")
X = "x"
FAR_Z = "z_far"
NEAR_Z = "z_near"
SHARD = (X, FAR_Z, NEAR_Z)
PLANE = (X, NEAR_Z)

MOMENTUM = 0.9
CLIP_RMS = 0.35
SQUARE_FLOOR = 0.0625
BLOCK = 16
F32 = jnp.float32
BF16 = jnp.bfloat16


def exchange(blocks, axis):
    return lax.all_to_all(blocks, axis, split_axis=0, concat_axis=0, tiled=True)


def spread(value, axis):
    return exchange(jnp.broadcast_to(value, (lax.axis_size(axis), *value.shape)), axis)


def whole_rows(shard):
    slots, rows, rank = shard.shape
    plane = spread(spread(shard, FAR_Z), PLANE)
    plane = plane.reshape(lax.axis_size(X), lax.axis_size(NEAR_Z), -1, slots, rows, rank)
    return plane.transpose(3, 0, 2, 1, 4, 5).reshape(slots, -1, rank)


def halves(value):
    high = value.astype(BF16)
    return high, (value - high.astype(F32)).astype(BF16)


def dot(a, b, dims):
    return lax.dot_general(a, b, (dims, ((), ())), preferred_element_type=F32)


VMEM = pl.BlockSpec(memory_space=pltpu.VMEM)


def pack_kernel(total_ref, proj_ref, pack_ref):
    slots, rows, n = proj_ref.shape
    row = lax.broadcasted_iota(jnp.int32, (n, n), 0)
    col = lax.broadcasted_iota(jnp.int32, (n, n), 1)
    grams = []
    for s in range(slots):
        high, low = halves(proj_ref[s])
        cross = dot(high, low, ((0,), (0,)))
        grams.append(dot(high, high, ((0,), (0,))) + (dot(low, low, ((0,), (0,))) + (cross + cross.T)))
    lower, upper = grams
    pack_ref[:, :n] = jnp.where(row >= col, lower, upper)
    diagonal = jnp.sum(jnp.where(row == col, upper, 0.0), axis=1, keepdims=True)
    row, col = row[:, :128], col[:, :128]
    totals = jnp.where(row == 0, total_ref[0], total_ref[1])
    pack_ref[:, n:] = jnp.where(col == 0, diagonal, jnp.where((col == 1) & (row < 2), totals, 0.0))


def packed_grams(proj, totals):
    rank = proj.shape[-1]
    return pl.pallas_call(
        pack_kernel,
        in_specs=[pl.BlockSpec(memory_space=pltpu.SMEM), VMEM],
        out_specs=VMEM,
        out_shape=jax.ShapeDtypeStruct((rank, rank + 128), F32),
        compiler_params=pltpu.CompilerParams(vmem_limit_bytes=12 << 20),
        name="packed_grams",
    )(totals, proj)


HBM = pl.BlockSpec(memory_space=pltpu.HBM)


def eliminate(work_ref, slots, n):
    b = BLOCK
    tiles = n // 128
    sub = lax.broadcasted_iota(jnp.int32, (b, 128), 0)
    sub_all = lax.broadcasted_iota(jnp.int32, (b, n), 0)
    lane_all = lax.broadcasted_iota(jnp.int32, (b, n), 1)
    for j in range(n // b):
        lo, hi = j * b, (j + 1) * b
        inside = (lane_all >= lo) & (lane_all < hi)
        panels = []
        cols = []
        for s in range(slots):
            panel = work_ref[s, lo:hi, :]
            cols.append([jnp.broadcast_to(panel[:, lo + k : lo + k + 1], (b, 128)) for k in range(b)])
            panels.append(jnp.where(inside, (lane_all - lo == sub_all).astype(F32), panel))
        for k in range(b):
            for s in range(slots):
                c = cols[s]
                inv = lax.rsqrt(jnp.broadcast_to(c[k][k : k + 1], (b, 128)))
                scaled = c[k] * inv
                below = jnp.where(sub > k, scaled, 0.0)
                for i in range(k + 1, b):
                    c[i] = c[i] - below * jnp.broadcast_to(scaled[i : i + 1], (b, 128))
                p = panels[s]
                pivot = p[k : k + 1] * jnp.concatenate([inv[:1]] * tiles, axis=1)
                below_all = jnp.concatenate([below] * tiles, axis=1)
                pivot_all = jnp.broadcast_to(pivot, (b, n))
                panels[s] = jnp.where(sub_all == k, pivot_all, p - below_all * pivot_all)
        for s in range(slots):
            work_ref[s, lo:hi, :] = panels[s]
            for f, g in ((hi, min(hi + b, n)), (hi + b, n)):
                if f < g:
                    update = lax.dot_general(
                        panels[s][:, f:g], panels[s], (((0,), (0,)), ((), ())),
                        precision=lax.Precision.HIGHEST, preferred_element_type=F32,
                    )
                    lane = lax.broadcasted_iota(jnp.int32, update.shape, 1)
                    old = jnp.where((lane >= lo) & (lane < hi), 0.0, work_ref[s, f:g, :])
                    work_ref[s, f:g, :] = old - update


def factor_kernel(near, scale, count_ref, pack_ref, proj_ref, buffer_ref, left_ref, half_ref, blocks_ref, work_ref, block_ref, sum_ref, sems):
    slots, rows, n = proj_ref.shape
    cols = block_ref.shape[-1]
    far, width = blocks_ref.shape[1], blocks_ref.shape[3]
    loads = [pltpu.make_async_copy(buffer_ref.at[s], block_ref.at[s], sems.at[s]) for s in range(slots)]
    for load in loads:
        load.start()
    row = lax.broadcasted_iota(jnp.int32, (n, n), 0)
    col = lax.broadcasted_iota(jnp.int32, (n, n), 1)
    squares, elements = pack_ref[:1, n + 1 : n + 2], pack_ref[1:2, n + 1 : n + 2]
    clip = jnp.minimum(1.0, CLIP_RMS * lax.rsqrt(jnp.maximum(squares / elements, SQUARE_FLOOR)))
    size = jnp.broadcast_to(clip * scale, (rows, n))
    pack = pack_ref[:, :n]
    turned = pack.T
    work_ref[0] = jnp.where(row >= col, pack, turned)
    diagonal = jnp.broadcast_to(pack_ref[:, n : n + 1], (n, n))
    work_ref[1] = jnp.where(row < col, pack, jnp.where(row > col, turned, diagonal))
    eliminate(work_ref, slots, n)
    for s in range(slots):
        high, low = halves(jnp.where(row >= col, work_ref[s], 0.0))
        proj_high, proj_low = halves(proj_ref[s])
        across = ((1,), (1,))
        ortho = dot(proj_high, high, across) + (dot(proj_high, low, across) + dot(proj_low, high, across))
        left_ref[s] = jnp.where(count_ref[0] > s, size * ortho, 0.0).astype(BF16)
        half = ortho.astype(BF16)
        half_ref[s] = half
        loads[s].wait()
        for c in range(0, cols, n):
            sum_ref[c : c + n, :] = dot(block_ref[s, :, c : c + n], half, ((0,), (0,)))
        for c in range(cols // width):
            x, z = divmod(c, far * near)
            f, m = divmod(z, near)
            blocks_ref[x * near + m, f, s] = sum_ref[c * width : (c + 1) * width, :].astype(BF16)


def factor(count, pack, proj, buffer, far, near, devices):
    slots, rows, rank = proj.shape
    cols = buffer.shape[-1]
    return pl.pallas_call(
        functools.partial(factor_kernel, near, math.sqrt(rows * devices)),
        in_specs=[pl.BlockSpec(memory_space=pltpu.SMEM), VMEM, VMEM, HBM],
        out_specs=[VMEM, VMEM, VMEM],
        out_shape=[
            jax.ShapeDtypeStruct((slots, rows, rank), BF16),
            jax.ShapeDtypeStruct((slots, rows, rank), BF16),
            jax.ShapeDtypeStruct((devices // far, far, slots, cols // devices, rank), BF16),
        ],
        scratch_shapes=[
            pltpu.VMEM((slots, rank, rank), F32),
            pltpu.VMEM((slots, rows, cols), BF16),
            pltpu.VMEM((cols, rank), F32),
            pltpu.SemaphoreType.DMA((slots,)),
        ],
        compiler_params=pltpu.CompilerParams(vmem_limit_bytes=32 << 20),
        name="factor",
    )(count, pack, proj, pltpu.with_memory_space_constraint(buffer, pltpu.HBM))


def add_kernel(blocks_ref, out_ref):
    for i in range(blocks_ref.shape[1]):
        total = blocks_ref[0, i].astype(F32)
        for j in range(1, blocks_ref.shape[0]):
            total = total + blocks_ref[j, i].astype(F32)
        out_ref[i] = total.astype(BF16)


def added(blocks):
    return pl.pallas_call(
        add_kernel,
        in_specs=[VMEM],
        out_specs=VMEM,
        out_shape=jax.ShapeDtypeStruct(blocks.shape[1:], BF16),
        compiler_params=pltpu.CompilerParams(vmem_limit_bytes=12 << 20),
        name="added",
    )(blocks)


def body(buffer, right_basis, layer_count):
    slots, rows_dev, cols = buffer.shape
    rank = right_basis.shape[-1]
    devices = lax.axis_size(SHARD)
    count = layer_count[0]
    used = jnp.arange(slots, dtype=jnp.int32) < count
    keep = used[:, None, None]

    basis = whole_rows(right_basis)
    squares = jnp.sum(jnp.square(buffer.astype(F32)), axis=(1, 2))
    squares = jnp.sum(jnp.where(used, squares, 0.0))
    elements = count.astype(F32) * float(rows_dev * cols)
    totals = lax.psum(jnp.stack([squares, elements]), SEG)
    proj = jnp.einsum("kij,kjr->kir", buffer, basis, preferred_element_type=F32)
    pack = packed_grams(proj, totals)
    part = exchange(pack.reshape(devices, -1, pack.shape[-1]), SHARD).sum(axis=0)
    pack = spread(part, SHARD).reshape(pack.shape)
    sizes = lax.axis_size(FAR_Z), lax.axis_size(NEAR_Z), devices
    left, half_left, blocks = factor(layer_count, pack, proj, buffer, *sizes)
    line = added(exchange(blocks, PLANE))
    right = exchange(line, FAR_Z).astype(F32).sum(axis=0)
    right, keep = lax.optimization_barrier((right, keep))
    half_right = whole_rows(right.astype(BF16))
    colsq = jnp.sum(jnp.square(half_right.astype(F32)), axis=1, keepdims=True)
    right_step = jnp.where(keep, right * (math.sqrt(cols) * lax.rsqrt(colsq + 1.0)), 0.0)

    correction = jnp.einsum("kir,kjr->kij", half_left, half_right, preferred_element_type=F32)
    moment = jnp.where(keep, buffer - (1.0 - MOMENTUM) * correction, 0.0).astype(BF16)
    return moment, left, right_step


def solution(mesh):
    split = Mesh(mesh.devices.reshape(4, 2, 4, 4, 2), (*SEG, *SHARD))
    specs = (P(SEG, SHARD, None), P(SEG, SHARD, None), P(SEG))
    outs = (P(SEG, SHARD, None),) * 3
    return jax.shard_map(body, mesh=split, in_specs=specs, out_specs=outs, check_vma=False)
```

```python
import functools
import math

import jax
import jax.numpy as jnp
from jax import lax
from jax.experimental import pallas as pl
from jax.experimental.pallas import tpu as pltpu
from jax.sharding import Mesh
from jax.sharding import PartitionSpec as P

SEG = ("segment_0", "segment_1")
X = "x"
FAR_Z = "z_far"
NEAR_Z = "z_near"
SHARD = (X, FAR_Z, NEAR_Z)
PLANE = (X, NEAR_Z)

MOMENTUM = 0.9
CLIP_RMS = 0.35
SQUARE_FLOOR = 0.0625
BLOCK = 16
F32 = jnp.float32
BF16 = jnp.bfloat16


def exchange(blocks, axis):
    return lax.all_to_all(blocks, axis, split_axis=0, concat_axis=0, tiled=True)


def spread(value, axis):
    return exchange(jnp.broadcast_to(value, (lax.axis_size(axis), *value.shape)), axis)


def whole_rows(line):
    slots, rows, rank = line.shape[1:]
    plane = spread(line, PLANE)
    plane = plane.reshape(lax.axis_size(X), lax.axis_size(NEAR_Z), -1, slots, rows, rank)
    return plane.transpose(3, 0, 2, 1, 4, 5).reshape(slots, -1, rank)


def halves(value):
    high = value.astype(BF16)
    return high, (value - high.astype(F32)).astype(BF16)


def dot(a, b, dims):
    return lax.dot_general(a, b, (dims, ((), ())), preferred_element_type=F32)


VMEM = pl.BlockSpec(memory_space=pltpu.VMEM)


def pack_kernel(total_ref, proj_ref, pack_ref):
    slots, rows, n = proj_ref.shape
    row = lax.broadcasted_iota(jnp.int32, (n, n), 0)
    col = lax.broadcasted_iota(jnp.int32, (n, n), 1)
    grams = []
    for s in range(slots):
        high, low = halves(proj_ref[s])
        cross = dot(high, low, ((0,), (0,)))
        grams.append(dot(high, high, ((0,), (0,))) + (dot(low, low, ((0,), (0,))) + (cross + cross.T)))
    lower, upper = grams
    pack_ref[:, :n] = jnp.where(row >= col, lower, upper)
    diagonal = jnp.sum(jnp.where(row == col, upper, 0.0), axis=1, keepdims=True)
    row, col = row[:, :128], col[:, :128]
    totals = jnp.where(row == 0, total_ref[0], total_ref[1])
    pack_ref[:, n:] = jnp.where(col == 0, diagonal, jnp.where((col == 1) & (row < 2), totals, 0.0))


def packed_grams(proj, totals):
    rank = proj.shape[-1]
    return pl.pallas_call(
        pack_kernel,
        in_specs=[pl.BlockSpec(memory_space=pltpu.SMEM), VMEM],
        out_specs=VMEM,
        out_shape=jax.ShapeDtypeStruct((rank, rank + 128), F32),
        compiler_params=pltpu.CompilerParams(vmem_limit_bytes=12 << 20),
        name="packed_grams",
    )(totals, proj)


HBM = pl.BlockSpec(memory_space=pltpu.HBM)


def eliminate(work_ref, slots, n):
    b = BLOCK
    tiles = n // 128
    sub = lax.broadcasted_iota(jnp.int32, (b, 128), 0)
    sub_all = lax.broadcasted_iota(jnp.int32, (b, n), 0)
    lane_all = lax.broadcasted_iota(jnp.int32, (b, n), 1)
    for j in range(n // b):
        lo, hi = j * b, (j + 1) * b
        inside = (lane_all >= lo) & (lane_all < hi)
        panels = []
        cols = []
        for s in range(slots):
            panel = work_ref[s, lo:hi, :]
            cols.append([jnp.broadcast_to(panel[:, lo + k : lo + k + 1], (b, 128)) for k in range(b)])
            panels.append(jnp.where(inside, (lane_all - lo == sub_all).astype(F32), panel))
        for k in range(b):
            for s in range(slots):
                c = cols[s]
                inv = lax.rsqrt(jnp.broadcast_to(c[k][k : k + 1], (b, 128)))
                scaled = c[k] * inv
                below = jnp.where(sub > k, scaled, 0.0)
                for i in range(k + 1, b):
                    c[i] = c[i] - below * jnp.broadcast_to(scaled[i : i + 1], (b, 128))
                p = panels[s]
                pivot = p[k : k + 1] * jnp.concatenate([inv[:1]] * tiles, axis=1)
                below_all = jnp.concatenate([below] * tiles, axis=1)
                pivot_all = jnp.broadcast_to(pivot, (b, n))
                panels[s] = jnp.where(sub_all == k, pivot_all, p - below_all * pivot_all)
        for s in range(slots):
            work_ref[s, lo:hi, :] = panels[s]
            for f, g in ((hi, min(hi + b, n)), (hi + b, n)):
                if f < g:
                    update = lax.dot_general(
                        panels[s][:, f:g], panels[s], (((0,), (0,)), ((), ())),
                        precision=lax.Precision.HIGHEST, preferred_element_type=F32,
                    )
                    lane = lax.broadcasted_iota(jnp.int32, update.shape, 1)
                    old = jnp.where((lane >= lo) & (lane < hi), 0.0, work_ref[s, f:g, :])
                    work_ref[s, f:g, :] = old - update


def factor_kernel(near, scale, count_ref, pack_ref, proj_ref, buffer_ref, left_ref, half_ref, blocks_ref, work_ref, block_ref, sum_ref, sems):
    slots, rows, n = proj_ref.shape
    cols = block_ref.shape[-1]
    far, width = blocks_ref.shape[1], blocks_ref.shape[3]
    loads = [pltpu.make_async_copy(buffer_ref.at[s], block_ref.at[s], sems.at[s]) for s in range(slots)]
    for load in loads:
        load.start()
    row = lax.broadcasted_iota(jnp.int32, (n, n), 0)
    col = lax.broadcasted_iota(jnp.int32, (n, n), 1)
    squares, elements = pack_ref[:1, n + 1 : n + 2], pack_ref[1:2, n + 1 : n + 2]
    clip = jnp.minimum(1.0, CLIP_RMS * lax.rsqrt(jnp.maximum(squares / elements, SQUARE_FLOOR)))
    size = jnp.broadcast_to(clip * scale, (rows, n))
    pack = pack_ref[:, :n]
    turned = pack.T
    work_ref[0] = jnp.where(row >= col, pack, turned)
    diagonal = jnp.broadcast_to(pack_ref[:, n : n + 1], (n, n))
    work_ref[1] = jnp.where(row < col, pack, jnp.where(row > col, turned, diagonal))
    eliminate(work_ref, slots, n)
    for s in range(slots):
        high, low = halves(jnp.where(row >= col, work_ref[s], 0.0))
        proj_high, proj_low = halves(proj_ref[s])
        across = ((1,), (1,))
        ortho = dot(proj_high, high, across) + (dot(proj_high, low, across) + dot(proj_low, high, across))
        left_ref[s] = jnp.where(count_ref[0] > s, size * ortho, 0.0).astype(BF16)
        half = ortho.astype(BF16)
        half_ref[s] = half
        loads[s].wait()
        for c in range(0, cols, n):
            sum_ref[c : c + n, :] = dot(block_ref[s, :, c : c + n], half, ((0,), (0,)))
        for c in range(cols // width):
            x, z = divmod(c, far * near)
            f, m = divmod(z, near)
            blocks_ref[x * near + m, f, s] = sum_ref[c * width : (c + 1) * width, :].astype(BF16)


def factor(count, pack, proj, buffer, far, near, devices):
    slots, rows, rank = proj.shape
    cols = buffer.shape[-1]
    return pl.pallas_call(
        functools.partial(factor_kernel, near, math.sqrt(rows * devices)),
        in_specs=[pl.BlockSpec(memory_space=pltpu.SMEM), VMEM, VMEM, HBM],
        out_specs=[VMEM, VMEM, VMEM],
        out_shape=[
            jax.ShapeDtypeStruct((slots, rows, rank), BF16),
            jax.ShapeDtypeStruct((slots, rows, rank), BF16),
            jax.ShapeDtypeStruct((devices // far, far, slots, cols // devices, rank), BF16),
        ],
        scratch_shapes=[
            pltpu.VMEM((slots, rank, rank), F32),
            pltpu.VMEM((slots, rows, cols), BF16),
            pltpu.VMEM((cols, rank), F32),
            pltpu.SemaphoreType.DMA((slots,)),
        ],
        compiler_params=pltpu.CompilerParams(vmem_limit_bytes=32 << 20),
        name="factor",
    )(count, pack, proj, pltpu.with_memory_space_constraint(buffer, pltpu.HBM))


def add_kernel(blocks_ref, out_ref):
    for i in range(blocks_ref.shape[1]):
        total = blocks_ref[0, i].astype(F32)
        for j in range(1, blocks_ref.shape[0]):
            total = total + blocks_ref[j, i].astype(F32)
        out_ref[i] = total.astype(BF16)


def added(blocks):
    return pl.pallas_call(
        add_kernel,
        in_specs=[VMEM],
        out_specs=VMEM,
        out_shape=jax.ShapeDtypeStruct(blocks.shape[1:], BF16),
        compiler_params=pltpu.CompilerParams(vmem_limit_bytes=12 << 20),
        name="added",
    )(blocks)


def body(buffer, right_basis, layer_count):
    slots, rows_dev, cols = buffer.shape
    rank = right_basis.shape[-1]
    devices = lax.axis_size(SHARD)
    count = layer_count[0]
    used = jnp.arange(slots, dtype=jnp.int32) < count
    keep = used[:, None, None]

    squares = jnp.sum(jnp.square(buffer.astype(F32)), axis=(1, 2))
    squares = jnp.sum(jnp.where(used, squares, 0.0))
    elements = count.astype(F32) * float(rows_dev * cols)
    totals = lax.psum(jnp.stack([squares, elements]), SEG)
    line, totals, keep = lax.optimization_barrier((spread(right_basis, FAR_Z), totals, keep))
    basis = whole_rows(line)
    proj = jnp.einsum("kij,kjr->kir", buffer, basis, preferred_element_type=F32)
    pack = packed_grams(proj, totals)
    part = exchange(pack.reshape(devices, -1, pack.shape[-1]), SHARD).sum(axis=0)
    pack = spread(part, SHARD).reshape(pack.shape)
    sizes = lax.axis_size(FAR_Z), lax.axis_size(NEAR_Z), devices
    left, half_left, blocks = factor(layer_count, pack, proj, buffer, *sizes)
    line = added(exchange(blocks, PLANE))
    right = exchange(line, FAR_Z).astype(F32).sum(axis=0)
    half_right = whole_rows(spread(right.astype(BF16), FAR_Z))
    colsq = jnp.sum(jnp.square(half_right.astype(F32)), axis=1, keepdims=True)
    right_step = jnp.where(keep, right * (math.sqrt(cols) * lax.rsqrt(colsq + 1.0)), 0.0)

    correction = jnp.einsum("kir,kjr->kij", half_left, half_right, preferred_element_type=F32)
    moment = jnp.where(keep, buffer - (1.0 - MOMENTUM) * correction, 0.0).astype(BF16)
    return moment, left, right_step


def solution(mesh):
    split = Mesh(mesh.devices.reshape(4, 2, 4, 4, 2), (*SEG, *SHARD))
    specs = (P(SEG, SHARD, None), P(SEG, SHARD, None), P(SEG))
    outs = (P(SEG, SHARD, None),) * 3
    return jax.shard_map(body, mesh=split, in_specs=specs, out_specs=outs, check_vma=False)
```
